32 devices in a mesh: src: 8 (over z, y), reg: 4 (over x, core).
Axes of the slice: x: 2, y: 2, z: 4, core: 2. Of those that a mesh axis runs over, the one named last changes fastest.
Arguments:
- tiles: bfloat16 [16384, 128, 128], P(('src', 'reg')), may hold values from -0.1875 to 0.1875
- rays: float32 [2048, 128], P(('src', 'reg')), may hold values from -6 to 6
- tile_rows: int32 [16384], P(('src', 'reg')), may hold values from 0 to 63, as said below
- tile_slots: int32 [16384], P(('src', 'reg')), may hold values from 0 to 63, as said below
- tile_count: int32 [32], P(('src', 'reg')), may hold values from 64 to 512, as said below
- wanted: int32 [32, 32, 2], P(('src', 'reg')), may hold values from 0 to 255
Outputs:
- solution: float32 [8192, 128], P(('src', 'reg'))
- right_vector: float32 [8192, 128], P(('src', 'reg'))
The draws below stay inside these ranges and needn't reach their ends.
Inputs may be any that keep to these rules, and one draw needn't show every extreme that they name: `tile_rows`: non-decreasing along each device's 512 tiles. `tile_slots`: the first 64 tiles of each device name every slot once. `tile_count`: some device has all 512 tiles live.
All inputs are finite; a program needn't handle non-finite values.
Results may differ from the reference program's by a relative error of at most 0.024.
Values may be sent and summed in bfloat16 or wider, within the bound.
A program may use at most 128 MiB of HBM per device.

```python
import jax
import jax.numpy as jnp
from jax import lax

TILE = 128
BLK_DEV = 256
RB_DEV = 64
TILE_SLOTS_EACH = 512
CAP = 2
ITERS = 3
NRAYBLK = 2048
NTILE = 16384
CELL_BLOCK_SLOTS = 64
DEVICES = 32


def draw_tile_rows(key, part):
    device_list = NTILE // TILE_SLOTS_EACH
    values = jax.random.randint(key, (device_list, TILE_SLOTS_EACH), 0, RB_DEV)
    return jnp.sort(values, axis=1).reshape(-1).astype(jnp.int32)


def draw_tile_slots(key, part):
    device_list = NTILE // TILE_SLOTS_EACH
    leading_part, trailing_part = jax.random.split(jax.random.fold_in(key, 7))
    random_keys = jax.random.split(leading_part, device_list)
    running_offsets = jax.vmap(lambda iteration_index: jax.random.permutation(iteration_index, CELL_BLOCK_SLOTS))(random_keys).astype(jnp.int32)
    remaining_part = jax.random.randint(trailing_part, (device_list, TILE_SLOTS_EACH - CELL_BLOCK_SLOTS), 0, CELL_BLOCK_SLOTS).astype(jnp.int32)
    return jnp.concatenate([running_offsets, remaining_part], axis=1).reshape(-1).astype(jnp.int32)


def draw_tile_count(key, part):
    leading_part, trailing_part = jax.random.split(key)
    device_list = NTILE // TILE_SLOTS_EACH
    entry_counts = jax.random.randint(leading_part, (device_list,), CELL_BLOCK_SLOTS, TILE_SLOTS_EACH + 1)
    filled = jax.random.randint(trailing_part, (), 0, device_list)
    return entry_counts.at[filled].set(TILE_SLOTS_EACH).astype(jnp.int32)


def touch_ends(entries, stream_key, low, top_value):
    spot = [jax.random.randint(jax.random.fold_in(stream_key, axis), (), 0, length) for axis, length in enumerate(entries.shape)]
    widest = entries.shape.index(max(entries.shape))
    beside = spot[:widest] + [(spot[widest] + 1) % entries.shape[widest]] + spot[widest + 1:]
    return entries.at[tuple(spot)].set(low).at[tuple(beside)].set(top_value)


def steps_of(stream_key, extent, pieces, smallest, high):
    gain = 1.0
    for position, shards_of in pieces:
        draws = jax.random.uniform(jax.random.fold_in(jax.random.fold_in(stream_key, 6), position), (shards_of,), jnp.float32, smallest / len(pieces), high / len(pieces))
        gain = gain * jnp.repeat(jnp.exp(draws), extent[position] // shards_of).reshape((-1,) + (1,) * (len(extent) - 1 - position))
    return gain


def scatter_about(own_key, extent, spread, limit, pieces=(), kind=jnp.bfloat16):
    values = spread * jax.random.normal(own_key, extent, jnp.float32)
    if pieces:
        values = values * steps_of(own_key, extent, pieces, -0.22, 0.18)
    return jnp.clip(values, -limit, limit).astype(kind)


def setup_inputs(seed: int = 0) -> dict:
    arg_keys = jax.random.split(jax.random.key(seed), 7)
    tiles = scatter_about(arg_keys[0], (NTILE, TILE, TILE), (TILE_SLOTS_EACH * TILE // RB_DEV) ** -0.5, 0.1875, ((0, 32),))
    rays = scatter_about(arg_keys[1], (NRAYBLK, TILE), 1.0, 6.0, ((0, 32),), jnp.float32)
    tile_rows = draw_tile_rows(jax.random.fold_in(arg_keys[6], 71), 0)
    tile_slots = draw_tile_slots(jax.random.fold_in(arg_keys[6], 71), 0)
    tile_count = draw_tile_count(jax.random.fold_in(arg_keys[6], 71), 0)
    wanted = touch_ends(jax.random.randint(arg_keys[5], (DEVICES, DEVICES, CAP), 0, BLK_DEV), jax.random.fold_in(arg_keys[5], 1), 0, BLK_DEV - 1).astype(jnp.int32)
    return {"tiles": tiles, "rays": rays, "tile_rows": tile_rows, "tile_slots": tile_slots, "tile_count": tile_count, "wanted": wanted}


damping = 0.5

def column_blocks(tile_slots, wanted, blocks_dev):
    device_list = wanted.shape[0]
    cap = wanted.shape[2]
    slots = tile_slots.reshape(device_list, -1)
    owner = slots // cap
    within = slots % cap
    asking = jnp.arange(device_list, dtype=jnp.int32)[:, None]
    local = wanted[owner, asking, within]
    return (owner * blocks_dev + local).astype(jnp.int32)

def forward(tiles4, vec_bf, columns, rows, live, row_blocks):

    def one(args):
        tile_set, cols, row_ids, mask = args
        picked = vec_bf[cols].astype(jnp.float32)
        prod = jnp.einsum('tij,tj->ti', tile_set.astype(jnp.float32), picked, precision=lax.Precision.HIGHEST)
        prod = prod * mask[:, None]
        return jax.ops.segment_sum(prod, row_ids, num_segments=row_blocks)
    result = lax.map(one, (tiles4, columns, rows, live))
    return result.reshape(-1, tiles4.shape[-1])

def adjoint(tiles4, ray_bf, columns, rows, live, total_blocks):
    device_list = tiles4.shape[0]
    width = tiles4.shape[-1]
    ray_dev = ray_bf.reshape(device_list, -1, width)

    def step(total, args):
        tile_set, cols, row_ids, mask, ray_set = args
        picked = ray_set[row_ids].astype(jnp.float32)
        contrib = jnp.einsum('tij,ti->tj', tile_set.astype(jnp.float32), picked, precision=lax.Precision.HIGHEST)
        contrib = contrib * mask[:, None]
        return (total.at[cols].add(contrib), None)
    start = jnp.zeros((total_blocks, width), jnp.float32)
    total, _ = lax.scan(step, start, (tiles4, columns, rows, live, ray_dev))
    return total

def reference(tiles, rays, tile_rows, tile_slots, tile_count, wanted):
    device_list = wanted.shape[0]
    width = tiles.shape[-1]
    total_blocks = BLK_DEV * device_list
    tiles4 = tiles.reshape(device_list, -1, width, width)
    per_dev = tiles4.shape[1]
    rows = tile_rows.reshape(device_list, per_dev)
    row_blocks = rays.shape[0] // device_list
    live = (jnp.arange(per_dev, dtype=jnp.int32)[None, :] < tile_count[:, None]).astype(jnp.float32)
    columns = column_blocks(tile_slots, wanted, BLK_DEV)
    u = jnp.zeros_like(rays)
    v = jnp.zeros((total_blocks, width), jnp.float32)
    solution = jnp.zeros((total_blocks, width), jnp.float32)
    w = jnp.zeros((total_blocks, width), jnp.float32)
    uraw = rays
    vraw = v
    alpha = jnp.float32(1.0)
    phibar = jnp.float32(0.0)
    rhobar = jnp.float32(0.0)
    for step in range(ITERS + 1):
        if step > 0:
            uraw = forward(tiles4, vraw.astype(jnp.bfloat16), columns, rows, live, row_blocks) / alpha - alpha * u
        beta = jnp.sqrt(jnp.sum(uraw * uraw))
        u = uraw / beta
        grad = adjoint(tiles4, uraw.astype(jnp.bfloat16), columns, rows, live, total_blocks)
        vraw = grad / beta - beta * v
        alpha_new = jnp.sqrt(jnp.sum(vraw * vraw))
        v_new = vraw / alpha_new
        if step == 0:
            w = v_new
            phibar = beta
            rhobar = alpha_new
        else:
            rhobar1 = jnp.sqrt(rhobar * rhobar + damping * damping)
            phibar = rhobar / rhobar1 * phibar
            rho = jnp.sqrt(rhobar1 * rhobar1 + beta * beta)
            cosine = rhobar1 / rho
            sine = beta / rho
            theta = sine * alpha_new
            rhobar = -cosine * alpha_new
            phi = cosine * phibar
            phibar = sine * phibar
            solution = solution + phi / rho * w
            w = v_new - theta / rho * w
        v = v_new
        alpha = alpha_new
    scale = jnp.sqrt(jnp.float32(total_blocks * width))
    return (solution, v * scale)
```

```python
import functools

import jax
import jax.numpy as jnp
from jax import lax
from jax.experimental import pallas as pl
from jax.experimental.pallas import tpu as pltpu
from jax.sharding import PartitionSpec as P

BLK_DEV = 256
ITERS = 3
damping = 0.5

QUARTERS = 4
CHUNKS = 16
F32 = jnp.float32
BF16 = jnp.bfloat16
MESH = pl.DeviceIdType.MESH
SIDE = 256


def kernel(
    n, regs, cap,
    count_ref, tiles_hbm, rays_ref, rows_ref, slots_ref, wanted_ref,
    sol_ref, right_ref,
    tiles_ref, turned_ref, index_vec, index_ref, goes_vec, goes_ref, plain_ref, ray_ref, cell_ref,
    key_send, key_recv, key_rows, same_ref, out_hot, inv_ref,
    vraw_ref, w_ref, update_ref, final_ref, final_recv,
    send_a, recv_a, norm_a, norm_recv_a, send_b, recv_b, norm_b, norm_recv_b,
    tile_sem, index_sem, send_sem, key_sem, a_sem, na_sem, b_sem, nb_sem, final_sem,
    acc_ray, acc_cell, acc_sum,
):
    src = lax.axis_index("src")
    reg = lax.axis_index("reg")
    me = src * regs + reg
    count = tiles_ref.shape[0]
    width = tiles_ref.shape[2]
    per_chunk = count // CHUNKS
    row_blocks = rays_ref.shape[0]
    steps = ITERS + 1
    chips = n // 2
    group = n // QUARTERS
    reducers = group // 2
    part = 2 * QUARTERS * cap
    slots_all = n * cap
    asked = n * part
    chip = me // 2
    core = lax.rem(me, 2)
    quarter = me // group
    place = lax.rem(chip, reducers)
    is_reducer = core == 1
    is_other = core == 0
    iota = functools.partial(lax.broadcasted_iota, jnp.int32)

    def tile_copy(c):
        span = pl.ds(c * per_chunk, per_chunk)
        return pltpu.make_async_copy(tiles_hbm.at[span], tiles_ref.at[span], tile_sem.at[c])

    for c in range(CHUNKS):
        tile_copy(c).start()

    def at(d):
        return (d // regs, lax.rem(d, regs))

    barrier = pltpu.get_barrier_semaphore()

    def greet(d):
        pl.semaphore_signal(barrier, inc=1, device_id=at(d), device_id_type=MESH)

    @pl.loop(1, chips)
    def _(k):
        greet(lax.rem(chip + k, chips) * 2 + 1)

    @pl.when(is_reducer)
    def _():
        @pl.loop(0, chips)
        def _(k):
            greet(lax.rem(chip + k, chips) * 2)

    @pl.when(is_other)
    def _():
        greet(me + 1)

    lines = rows_ref.shape[0]
    tile_id = iota((lines, width), 0) * width + iota((lines, width), 1)
    live = tile_id < count_ref[...]
    slots = slots_ref[...]
    owner = slots // cap
    within = lax.rem(owner, group)
    spot = (within // 2) * part + (2 * (owner // group) + lax.rem(within, 2)) * cap + lax.rem(slots, cap)
    index_vec[:lines, :] = jnp.where(live, rows_ref[...], row_blocks)
    index_vec[lines:, :] = jnp.where(live, spot, slots_all)
    goes_vec[...] = index_vec[...].astype(F32)
    index_copies = (
        pltpu.make_async_copy(index_vec, index_ref, index_sem.at[0]),
        pltpu.make_async_copy(goes_vec, goes_ref, index_sem.at[1]),
    )
    for copy in index_copies:
        copy.start()

    asks = wanted_ref[...].astype(F32)
    lane = iota((1, asked), 1)
    asker = iota((cap, asked), 1) // part
    spread = jnp.zeros((cap, asked), F32)
    for d in range(n):
        spread = jnp.where(asker == d, asks[:, d : d + 1], spread)
    which = 2 * quarter + core
    keys = jnp.zeros((1, asked), F32)
    for k in range(cap):
        hit = lax.rem(lane, part) == which * cap + k
        keys = keys + jnp.where(hit, spread[k : k + 1] + (which * BLK_DEV).astype(F32), 0.0)
    key_send[...] = keys

    for acc in (*acc_ray, *acc_cell, *acc_sum):
        pltpu.matmul_pop(acc)

    ray_ref[row_blocks] = jnp.zeros((16, width), BF16)
    cell_ref[slots_all] = jnp.zeros((16, width), BF16)

    def spread_rows(vec_ref, value):
        plain_ref[pl.ds(0, value.shape[0]), :] = value
        for r in range(value.shape[0]):
            row = plain_ref[pl.ds(r, 8, stride=0), :]
            vec_ref[r] = jnp.concatenate([row, row], axis=0).astype(BF16)

    def left_of(vec_ref, rows_out, base_in, base_out, g, i):
        value = vec_ref[index_ref[base_in + g, i]]
        value = jnp.concatenate([value] * (rows_out // 16), axis=0)
        goes = jnp.broadcast_to(goes_ref[base_out + g, i], (16, width)).astype(BF16)
        goes = jnp.concatenate([goes] * (rows_out // 16), axis=0)
        hot = iota((rows_out, width), 0).astype(F32).astype(BF16) == goes
        return jnp.where(hot, value, jnp.zeros_like(value))

    def feed(source, vec_ref, accs, base_in, base_out, g, t, q, register):
        tile = [source[g * width + t + i] for i in range(4)]
        right = jnp.concatenate(
            [jnp.concatenate(tile[:2], axis=1), jnp.concatenate(tile[2:], axis=1)], axis=0
        )
        rows_out = accs[0].shape[0]
        left = [left_of(vec_ref, rows_out, base_in, base_out, g, t + i) for i in range(4)]
        pltpu.matmul_push_rhs(right, staging_register=register, mxu_index=q)
        pltpu.matmul_acc_lhs(
            accs[2 * q], jnp.concatenate([left[0], left[2]], axis=1), load_staged_rhs=register
        )
        pltpu.matmul_acc_lhs(accs[2 * q + 1], jnp.concatenate([left[1], left[3]], axis=1))

    def feed_many(source, vec_ref, accs, base_in, base_out, g, t, pairs):
        for i in range(pairs):
            for q in range(2):
                feed(source, vec_ref, accs, base_in, base_out, g, t + 8 * i + 4 * q, q, i % 2)

    def taken(accs):
        pieces = [pltpu.matmul_pop(acc) for acc in accs]
        return (pieces[0][:, :width] + pieces[2][:, :width]) + (
            pieces[1][:, width:] + pieces[3][:, width:]
        )

    def full_pass(source, vec_ref, accs, base_in, base_out):
        @pl.loop(0, lines)
        def _(g):
            feed_many(source, vec_ref, accs, base_in, base_out, g, 0, width // 8)

        return taken(accs)

    def product(left_ref, right_of, use):
        high, deep = left_ref.shape
        for m in range(0, high, 2 * SIDE):
            for k in range(0, deep, SIDE):
                for p, right in enumerate(right_of(k)):
                    for q in range(2):
                        pltpu.matmul_push_rhs(right, staging_register=p % 2, mxu_index=q)
                        pltpu.matmul_acc_lhs(
                            acc_sum[q],
                            left_ref[pl.ds(m + q * SIDE, SIDE), pl.ds(k, SIDE)],
                            load_staged_rhs=p % 2,
                        )
            for q in range(2):
                use(m + q * SIDE, pltpu.matmul_pop(acc_sum[q]))

    def remote(source, target, sem, d):
        return pltpu.make_async_remote_copy(
            src_ref=source, dst_ref=target, send_sem=send_sem, recv_sem=sem,
            device_id=at(d), device_id_type=MESH,
        )

    def wait_for(ref, number, sem):
        ref = ref.at[pl.ds(0, number)]
        pltpu.make_async_copy(ref, ref, sem).wait()

    def total(x):
        return jnp.sum(x, keepdims=True)

    def send_keys():
        for k in range(QUARTERS):
            d = lax.rem(quarter + k, QUARTERS) * group + 2 * place + 1
            copy = remote(key_send, key_recv.at[which], key_sem, d)
            if k > 0:
                copy.start()
            else:
                pl.when(is_other)(copy.start)

    def send_sums(step):
        for k in range(chips - 1, -1, -1):
            to = chip ^ k if chips & (chips - 1) == 0 else lax.rem(chip + k, chips)
            d = 2 * to + 1
            copies = (
                remote(send_a.at[step, lax.rem(to, reducers)], recv_a.at[step, me], a_sem.at[step], d),
                remote(norm_a.at[step], norm_recv_a.at[step, me], na_sem.at[step], d),
            )

            def start(copies=copies):
                for copy in copies:
                    copy.start()

            if k > 0:
                start()
            else:
                pl.when(is_other)(start)

    def send_back(step, data):
        for k in range(group - 1, 0, -1):
            local = (
                lax.rem(me, group) ^ k if group & (group - 1) == 0 else lax.rem(me + k, group)
            )
            d = quarter * group + local
            if data:
                remote(send_b.at[step, local], recv_b.at[step, place], b_sem.at[step], d).start()
            remote(norm_b.at[step], norm_recv_b.at[step, place], nb_sem.at[step], d).start()

    def prepare():
        wait_for(key_recv, 2 * QUARTERS - 1, key_sem)
        key_recv[which] = key_send[...]
        row = jnp.sum(key_recv[...], axis=0)
        key_rows[...] = jnp.broadcast_to(row, key_rows.shape)
        for b in range(0, asked, width):
            block = key_rows[:, pl.ds(b, width)]
            column = jnp.concatenate([block] * (width // 8), axis=0).T
            times = jnp.zeros((width, width), F32)
            for c in range(0, asked, width):
                equal = jnp.where(column == key_rows[pl.ds(0, 1), pl.ds(c, width)], 1.0, 0.0)
                same_ref[pl.ds(b, width), pl.ds(c, width)] = equal.astype(BF16)
                times = times + equal
            times = jnp.sum(times, axis=1, keepdims=True)
            inv_ref[pl.ds(b, width), :] = jnp.broadcast_to(1.0 / times, (width, width))

    def prepare_out():
        first = (2 * quarter * BLK_DEV).astype(F32)
        high = out_hot.shape[0]
        number = iota((high, width), 0).astype(F32) + first
        for c in range(0, asked, width):
            equal = jnp.where(number == key_rows[pl.ds(0, 1), pl.ds(c, width)], 1.0, 0.0)
            out_hot[:, pl.ds(c, width)] = equal.astype(BF16)

    def turn():
        @pl.loop(0, count // 16)
        def _(g):
            for i in range(16):
                turned_ref[g * 16 + i] = tiles_ref[g * 16 + i].T

    u = None
    alpha = phibar = rhobar = None
    coefs = None
    uraw = rays_ref[...]
    for step in range(steps):
        if step > 0:
            spread_rows(cell_ref, recv_b[step - 1].reshape(slots_all, width).astype(F32))
            uraw = full_pass(turned_ref, cell_ref, acc_ray, lines, 0) / alpha - alpha * u
            spread_rows(ray_ref, uraw)
            sums = full_pass(tiles_ref, ray_ref, acc_cell, 0, lines)
        else:
            spread_rows(ray_ref, uraw)
            for copy in index_copies:
                copy.wait()
            per_line = width // per_chunk

            @pl.loop(0, lines)
            def _(g):
                for c in range(per_line):
                    tile_copy(g * per_line + c).wait()
                    feed_many(tiles_ref, ray_ref, acc_cell, 0, lines, g, c * per_chunk, per_chunk // 8)

            sums = taken(acc_cell)
        send_a[step] = sums.astype(BF16).reshape(reducers, part, width)
        norm_a[step] = jnp.sum(uraw * uraw, axis=0, keepdims=True)
        if step == 0:
            pl.when(is_reducer)(lambda: pl.semaphore_wait(barrier, n - 1))
            pl.when(is_other)(lambda: pl.semaphore_wait(barrier, chips))
            send_keys()
        send_sums(step)

        @pl.when(is_reducer)
        def _(step=step, alpha=alpha, phibar=phibar, rhobar=rhobar, coefs=coefs):
            recv_a[step, me] = send_a[step, place]
            norm_recv_a[step, me] = norm_a[step]
            if step == 0:
                prepare()
            else:
                v = vraw_ref[...] / alpha
                if step == 1:
                    w_ref[...] = v
                    update_ref[...] = jnp.zeros_like(v)
                else:
                    w = w_ref[...]
                    update_ref[...] = update_ref[...] + coefs[0] * w
                    w_ref[...] = v - coefs[1] * w
            if step == 1:
                prepare_out()

        if step == 0:
            turn()

        @pl.when(is_reducer)
        def _(step=step, alpha=alpha, phibar=phibar, rhobar=rhobar):
            wait_for(norm_recv_a.at[step], n - 1, na_sem.at[step])
            wait_for(recv_a.at[step], n - 1, a_sem.at[step])
            beta = jnp.sqrt(total(jnp.sum(norm_recv_a[step], axis=0)))

            def pieces(k):
                got = recv_a[step, pl.ds(k // part, SIDE // part)].reshape(SIDE, width)
                return (jnp.concatenate([got, got], axis=1),)

            squares = []

            def use(m, value):
                span = pl.ds(m, SIDE)
                vraw = value[:, :width] / beta
                if step > 0:
                    vraw = vraw - (beta / alpha) * vraw_ref[span, :]
                vraw_ref[span, :] = vraw
                squares.append(jnp.sum(vraw * vraw * inv_ref[span, :], axis=0, keepdims=True))

            product(same_ref, pieces, use)
            norm_b[step, pl.ds(0, 1), :] = functools.reduce(jnp.add, squares)
            norm_b[step, pl.ds(1, 1), :] = jnp.broadcast_to(beta, (1, width))
            if step < steps - 1:
                own = vraw_ref[pl.ds(pl.multiple_of(quarter * group * part, 8), group * part), :]
                send_b[step] = own.astype(BF16).reshape(group, part, width)
            send_back(step, step < steps - 1)
            norm_recv_b[step, place] = norm_b[step]
            if step < steps - 1:
                recv_b[step, place] = send_b[step, lax.rem(me, group)]
            else:
                rhobar1 = jnp.sqrt(rhobar * rhobar + damping * damping)
                rho = jnp.sqrt(rhobar1 * rhobar1 + beta * beta)
                scale = (rhobar1 / rho) * ((rhobar / rhobar1) * phibar) / rho
                update = (update_ref[...] + scale * w_ref[...]) * inv_ref[...]
                update_ref[...] = update
                vraw_ref[...] = vraw_ref[...] * inv_ref[...]

                def parts(k):
                    span = pl.ds(k, SIDE)
                    x = jnp.concatenate([update_ref[span, :], vraw_ref[span, :]], axis=1)
                    high = x.astype(BF16)
                    return high, (x - high.astype(F32)).astype(BF16)

                def use_final(m, value):
                    final_ref[m // SIDE] = value

                product(out_hot, parts, use_final)
                remote(final_ref.at[0], final_recv.at[0], final_sem, me - 1).start()
            wait_for(norm_recv_b.at[step], reducers - 1, nb_sem.at[step])
            if step < steps - 1:
                wait_for(recv_b.at[step], reducers - 1, b_sem.at[step])

        @pl.when(is_other)
        def _(step=step):
            wait_for(norm_recv_b.at[step], reducers, nb_sem.at[step])
            if step < steps - 1:
                wait_for(recv_b.at[step], reducers, b_sem.at[step])

        alpha = jnp.sqrt(total(jnp.sum(norm_recv_b[step], axis=0)[:1]))
        beta = norm_recv_b[step, 0, pl.ds(1, 1), pl.ds(0, 1)]
        u = uraw / beta
        if step == 0:
            phibar = beta
            rhobar = alpha
        else:
            rhobar1 = jnp.sqrt(rhobar * rhobar + damping * damping)
            phibar = rhobar / rhobar1 * phibar
            rho = jnp.sqrt(rhobar1 * rhobar1 + beta * beta)
            cosine = rhobar1 / rho
            sine = beta / rho
            theta = sine * alpha
            rhobar = -cosine * alpha
            phi = cosine * phibar
            phibar = sine * phibar
            coefs = (phi / rho, theta / rho)

    blocks = sol_ref.shape[0]
    scale = float(blocks * width * n) ** 0.5 / alpha

    def put(result):
        sol_ref[...] = result[:, :width]
        right_ref[...] = result[:, width:] * scale

    @pl.when(is_reducer)
    def _():
        put(final_ref[1])

    @pl.when(is_other)
    def _():
        wait_for(final_recv, 1, final_sem)
        put(final_recv[0])

    @pl.when(is_reducer)
    def _():
        for k in range(QUARTERS - 1):
            wait_for(key_recv, 1, send_sem)
        for step in range(steps):
            wait_for(recv_a.at[step], chips - 1, send_sem)
            wait_for(norm_recv_a.at[step], chips - 1, send_sem)
            wait_for(norm_b.at[pl.ds(0, 1)], 1, send_sem) if group == 2 else None
            for k in range(group - 1):
                wait_for(norm_recv_b.at[step], 1, send_sem)
                if step < steps - 1:
                    wait_for(recv_b.at[step], 1, send_sem)
        wait_for(final_recv, 1, send_sem)

    @pl.when(is_other)
    def _():
        for k in range(QUARTERS):
            wait_for(key_recv, 1, send_sem)
        for step in range(steps):
            wait_for(recv_a.at[step], chips, send_sem)
            wait_for(norm_recv_a.at[step], chips, send_sem)


def per_device(n, regs, tiles, rays, tile_rows, tile_slots, tile_count, wanted):
    count, width = tiles.shape[0], tiles.shape[2]
    cap = wanted.shape[2]
    steps = ITERS + 1
    row_blocks = rays.shape[0]
    group = n // QUARTERS
    reducers = group // 2
    part = 2 * QUARTERS * cap
    slots_all = n * cap
    asked = n * part
    lines = count // width
    vmem = pl.BlockSpec(memory_space=pltpu.VMEM)
    out = jax.ShapeDtypeStruct((BLK_DEV, width), F32)

    def body(*refs):
        def inner(acc_ray, acc_cell, acc_sum):
            kernel(n, regs, cap, *refs, acc_ray, acc_cell, acc_sum)

        def four(rows):
            return tuple(pltpu.ACC(q)((rows, SIDE), F32) for q in (0, 0, 1, 1))

        pl.run_scoped(
            inner, four(row_blocks), four(slots_all),
            tuple(pltpu.ACC(q)((SIDE, SIDE), F32) for q in (0, 1)),
        )

    return pl.pallas_call(
        body,
        out_shape=(out, out),
        in_specs=[vmem, pl.BlockSpec(memory_space=pl.ANY)] + [vmem] * 4,
        out_specs=(vmem, vmem),
        scratch_shapes=[
            pltpu.VMEM(tiles.shape, BF16),
            pltpu.VMEM(tiles.shape, BF16),
            pltpu.VMEM((2 * lines, width), jnp.int32),
            pltpu.SMEM((2 * lines, width), jnp.int32),
            pltpu.VMEM((2 * lines, width), F32),
            pltpu.SMEM((2 * lines, width), F32),
            pltpu.VMEM((max(row_blocks, slots_all) + 8, width), F32),
            pltpu.VMEM((row_blocks + 1, 16, width), BF16),
            pltpu.VMEM((slots_all + 1, 16, width), BF16),
            pltpu.VMEM((1, asked), F32),
            pltpu.VMEM((2 * QUARTERS, 1, asked), F32),
            pltpu.VMEM((8, asked), F32),
            pltpu.VMEM((asked, asked), BF16),
            pltpu.VMEM((2 * BLK_DEV, asked), BF16),
            pltpu.VMEM((asked, width), F32),
            pltpu.VMEM((asked, width), F32),
            pltpu.VMEM((asked, width), F32),
            pltpu.VMEM((asked, width), F32),
            pltpu.VMEM((2, BLK_DEV, 2 * width), F32),
            pltpu.VMEM((1, BLK_DEV, 2 * width), F32),
            pltpu.VMEM((steps, reducers, part, width), BF16),
            pltpu.VMEM((steps, n, part, width), BF16),
            pltpu.VMEM((steps, 1, width), F32),
            pltpu.VMEM((steps, n, 1, width), F32),
            pltpu.VMEM((steps - 1, group, part, width), BF16),
            pltpu.VMEM((steps - 1, reducers, part, width), BF16),
            pltpu.VMEM((steps, 2, width), F32),
            pltpu.VMEM((steps, reducers, 2, width), F32),
            pltpu.SemaphoreType.DMA((CHUNKS,)),
            pltpu.SemaphoreType.DMA((2,)),
            pltpu.SemaphoreType.DMA,
            pltpu.SemaphoreType.DMA,
            pltpu.SemaphoreType.DMA((steps,)),
            pltpu.SemaphoreType.DMA((steps,)),
            pltpu.SemaphoreType.DMA((steps,)),
            pltpu.SemaphoreType.DMA((steps,)),
            pltpu.SemaphoreType.DMA,
        ],
        compiler_params=pltpu.CompilerParams(
            collective_id=0, has_side_effects=True, vmem_limit_bytes=56 * 1024 * 1024
        ),
    )(
        tile_count[None, :],
        tiles,
        rays,
        tile_rows.reshape(lines, width),
        tile_slots.reshape(lines, width),
        wanted[0].T,
    )


def solution(mesh):
    both = ("src", "reg")
    in_specs = (
        P(both, None, None),
        P(both, None),
        P(both),
        P(both),
        P(both),
        P(both, None, None),
    )
    out_specs = (P(both, None), P(both, None))
    n = mesh.shape["src"] * mesh.shape["reg"]
    return jax.shard_map(
        functools.partial(per_device, n, mesh.shape["reg"]),
        mesh=mesh,
        in_specs=in_specs,
        out_specs=out_specs,
        check_vma=False,
    )
```

```python
import functools

import jax
import jax.numpy as jnp
from jax import lax
from jax.experimental import pallas as pl
from jax.experimental.pallas import tpu as pltpu
from jax.sharding import PartitionSpec as P

BLK_DEV = 256
ITERS = 3
damping = 0.5

QUARTERS = 4
CHUNKS = 16
AHEAD = 6
F32 = jnp.float32
BF16 = jnp.bfloat16
MESH = pl.DeviceIdType.MESH
SIDE = 256


def kernel(
    n, regs, cap,
    count_hbm, tiles_hbm, rays_hbm, rows_hbm, slots_hbm, wanted_hbm,
    result_ref,
    count_ref, rays_ref, rows_ref, slots_ref, wanted_ref,
    tiles_ref, turned_ref, index_vec, index_ref, goes_vec, goes_ref, plain_ref, ray_ref, cell_ref,
    key_send, key_recv, key_rows, same_ref, out_hot, inv_ref,
    vraw_ref, w_ref, update_ref, final_ref, final_recv,
    send_a, recv_a, norm_a, norm_recv_a, send_b, recv_b, norm_b, norm_recv_b,
    tile_sem, input_sem, index_sem, send_sem, key_sem, a_sem, na_sem, b_sem, nb_sem, final_sem,
    acc_ray, acc_cell, acc_sum,
):
    src = lax.axis_index("src")
    reg = lax.axis_index("reg")
    me = src * regs + reg
    count = tiles_ref.shape[0]
    width = tiles_ref.shape[2]
    per_chunk = count // CHUNKS
    row_blocks = rays_ref.shape[0]
    steps = ITERS + 1
    chips = n // 2
    group = n // QUARTERS
    reducers = group // 2
    part = 2 * QUARTERS * cap
    slots_all = n * cap
    asked = n * part
    chip = me // 2
    core = lax.rem(me, 2)
    quarter = me // group
    place = lax.rem(chip, reducers)
    is_reducer = core == 1
    is_other = core == 0
    iota = functools.partial(lax.broadcasted_iota, jnp.int32)

    def tile_copy(c):
        span = pl.ds(c * per_chunk, per_chunk)
        return pltpu.make_async_copy(tiles_hbm.at[span], tiles_ref.at[span], tile_sem.at[c])

    inputs = [
        pltpu.make_async_copy(a, b, input_sem.at[i])
        for i, (a, b) in enumerate((
            (count_hbm, count_ref), (rows_hbm, rows_ref), (slots_hbm, slots_ref),
            (rays_hbm, rays_ref), (wanted_hbm, wanted_ref),
        ))
    ]
    for copy in inputs:
        copy.start()
    for c in range(AHEAD):
        tile_copy(c).start()

    def at(d):
        return (d // regs, lax.rem(d, regs))

    barrier = pltpu.get_barrier_semaphore()

    def greet(d):
        pl.semaphore_signal(barrier, inc=1, device_id=at(d), device_id_type=MESH)

    @pl.loop(1, chips)
    def _(k):
        greet(lax.rem(chip + k, chips) * 2 + 1)

    @pl.when(is_reducer)
    def _():
        @pl.loop(0, chips)
        def _(k):
            greet(lax.rem(chip + k, chips) * 2)

    @pl.when(is_other)
    def _():
        greet(me + 1)

    for copy in inputs:
        copy.wait()
    lines = rows_ref.shape[0]
    tile_id = iota((lines, width), 0) * width + iota((lines, width), 1)
    live = tile_id < count_ref[0]
    slots = slots_ref[...]
    owner = slots // cap
    within = lax.rem(owner, group)
    spot = (within // 2) * part + (2 * (owner // group) + lax.rem(within, 2)) * cap + lax.rem(slots, cap)
    index_vec[:lines, :] = jnp.where(live, rows_ref[...], row_blocks)
    index_vec[lines:, :] = jnp.where(live, spot, slots_all)
    goes_vec[...] = index_vec[...].astype(F32)
    index_copies = (
        pltpu.make_async_copy(index_vec, index_ref, index_sem.at[0]),
        pltpu.make_async_copy(goes_vec, goes_ref, index_sem.at[1]),
    )
    for copy in index_copies:
        copy.start()

    asks = wanted_ref[...].astype(F32)
    lane = iota((1, asked), 1)
    asker = iota((cap, asked), 1) // part
    spread = jnp.zeros((cap, asked), F32)
    for d in range(n):
        spread = jnp.where(asker == d, asks[:, d : d + 1], spread)
    which = 2 * quarter + core
    keys = jnp.zeros((1, asked), F32)
    for k in range(cap):
        hit = lax.rem(lane, part) == which * cap + k
        keys = keys + jnp.where(hit, spread[k : k + 1] + (which * BLK_DEV).astype(F32), 0.0)
    key_send[...] = keys

    for acc in (*acc_ray, *acc_cell, *acc_sum):
        pltpu.matmul_pop(acc)

    ray_ref[row_blocks] = jnp.zeros((16, width), BF16)
    cell_ref[slots_all] = jnp.zeros((16, width), BF16)

    def spread_rows(vec_ref, value):
        plain_ref[pl.ds(0, value.shape[0]), :] = value
        for r in range(value.shape[0]):
            row = plain_ref[pl.ds(r, 8, stride=0), :]
            vec_ref[r] = jnp.concatenate([row, row], axis=0).astype(BF16)

    def left_of(vec_ref, rows_out, base_in, base_out, g, i):
        value = vec_ref[index_ref[base_in + g, i]]
        value = jnp.concatenate([value] * (rows_out // 16), axis=0)
        goes = jnp.broadcast_to(goes_ref[base_out + g, i], (16, width)).astype(BF16)
        goes = jnp.concatenate([goes] * (rows_out // 16), axis=0)
        hot = iota((rows_out, width), 0).astype(F32).astype(BF16) == goes
        return jnp.where(hot, value, jnp.zeros_like(value))

    def feed(source, vec_ref, accs, base_in, base_out, g, t, q, register):
        tile = [source[g * width + t + i] for i in range(4)]
        right = jnp.concatenate(
            [jnp.concatenate(tile[:2], axis=1), jnp.concatenate(tile[2:], axis=1)], axis=0
        )
        rows_out = accs[0].shape[0]
        left = [left_of(vec_ref, rows_out, base_in, base_out, g, t + i) for i in range(4)]
        pltpu.matmul_push_rhs(right, staging_register=register, mxu_index=q)
        pltpu.matmul_acc_lhs(
            accs[2 * q], jnp.concatenate([left[0], left[2]], axis=1), load_staged_rhs=register
        )
        pltpu.matmul_acc_lhs(accs[2 * q + 1], jnp.concatenate([left[1], left[3]], axis=1))

    def feed_many(source, vec_ref, accs, base_in, base_out, g, t, pairs):
        for i in range(pairs):
            for q in range(2):
                feed(source, vec_ref, accs, base_in, base_out, g, t + 8 * i + 4 * q, q, i % 2)

    def taken(accs):
        pieces = [pltpu.matmul_pop(acc) for acc in accs]
        return (pieces[0][:, :width] + pieces[2][:, :width]) + (
            pieces[1][:, width:] + pieces[3][:, width:]
        )

    def full_pass(source, vec_ref, accs, base_in, base_out):
        @pl.loop(0, lines)
        def _(g):
            feed_many(source, vec_ref, accs, base_in, base_out, g, 0, width // 8)

        return taken(accs)

    def product(left_ref, right_of, use):
        high, deep = left_ref.shape
        for m in range(0, high, 2 * SIDE):
            for k in range(0, deep, SIDE):
                for p, right in enumerate(right_of(k)):
                    for q in range(2):
                        pltpu.matmul_push_rhs(right, staging_register=p % 2, mxu_index=q)
                        pltpu.matmul_acc_lhs(
                            acc_sum[q],
                            left_ref[pl.ds(m + q * SIDE, SIDE), pl.ds(k, SIDE)],
                            load_staged_rhs=p % 2,
                        )
            for q in range(2):
                use(m + q * SIDE, pltpu.matmul_pop(acc_sum[q]))

    def remote(source, target, sem, d):
        return pltpu.make_async_remote_copy(
            src_ref=source, dst_ref=target, send_sem=send_sem, recv_sem=sem,
            device_id=at(d), device_id_type=MESH,
        )

    def wait_for(ref, number, sem):
        ref = ref.at[pl.ds(0, number)]
        pltpu.make_async_copy(ref, ref, sem).wait()

    def total(x):
        return jnp.sum(x, keepdims=True)

    def send_keys():
        for k in range(QUARTERS):
            d = lax.rem(quarter + k, QUARTERS) * group + 2 * place + 1
            copy = remote(key_send, key_recv.at[which], key_sem, d)
            if k > 0:
                copy.start()
            else:
                pl.when(is_other)(copy.start)

    def send_sums(step):
        for k in range(chips - 1, -1, -1):
            to = chip ^ k if chips & (chips - 1) == 0 else lax.rem(chip + k, chips)
            d = 2 * to + 1
            copies = (
                remote(send_a.at[step, lax.rem(to, reducers)], recv_a.at[step, me], a_sem.at[step], d),
                remote(norm_a.at[step], norm_recv_a.at[step, me], na_sem.at[step], d),
            )

            def start(copies=copies):
                for copy in copies:
                    copy.start()

            if k > 0:
                start()
            else:
                pl.when(is_other)(start)

    def send_back(step, data):
        for k in range(group - 1, 0, -1):
            local = (
                lax.rem(me, group) ^ k if group & (group - 1) == 0 else lax.rem(me + k, group)
            )
            d = quarter * group + local
            if data:
                remote(send_b.at[step, local], recv_b.at[step, place], b_sem.at[step], d).start()
            remote(norm_b.at[step], norm_recv_b.at[step, place], nb_sem.at[step], d).start()

    def prepare():
        wait_for(key_recv, 2 * QUARTERS - 1, key_sem)
        key_recv[which] = key_send[...]
        row = jnp.sum(key_recv[...], axis=0)
        key_rows[...] = jnp.broadcast_to(row, key_rows.shape)
        for b in range(0, asked, width):
            block = key_rows[:, pl.ds(b, width)]
            column = jnp.concatenate([block] * (width // 8), axis=0).T
            times = jnp.zeros((width, width), F32)
            for c in range(0, asked, width):
                equal = jnp.where(column == key_rows[pl.ds(0, 1), pl.ds(c, width)], 1.0, 0.0)
                same_ref[pl.ds(b, width), pl.ds(c, width)] = equal.astype(BF16)
                times = times + equal
            times = jnp.sum(times, axis=1, keepdims=True)
            inv_ref[pl.ds(b, width), :] = jnp.broadcast_to(1.0 / times, (width, width))

    def prepare_out():
        first = (2 * quarter * BLK_DEV).astype(F32)
        high = out_hot.shape[0]
        number = iota((high, width), 0).astype(F32) + first
        for c in range(0, asked, width):
            equal = jnp.where(number == key_rows[pl.ds(0, 1), pl.ds(c, width)], 1.0, 0.0)
            out_hot[:, pl.ds(c, width)] = equal.astype(BF16)

    early = per_chunk // 2

    def turn(first, number):
        for i in range(number):
            turned_ref[first + i] = tiles_ref[first + i].T

    def turn_rest():
        @pl.loop(0, CHUNKS)
        def _(c):
            turn(c * per_chunk + early, per_chunk - early)

    u = None
    alpha = phibar = rhobar = None
    coefs = None
    uraw = rays_ref[...]
    for step in range(steps):
        if step > 0:
            spread_rows(cell_ref, recv_b[step - 1].reshape(slots_all, width).astype(F32))
            uraw = full_pass(turned_ref, cell_ref, acc_ray, lines, 0) / alpha - alpha * u
            spread_rows(ray_ref, uraw)
            sums = full_pass(tiles_ref, ray_ref, acc_cell, 0, lines)
        else:
            spread_rows(ray_ref, uraw)
            for copy in index_copies:
                copy.wait()
            per_line = width // per_chunk

            def line(g):
                for c in range(per_line):
                    if g * per_line + c + AHEAD < CHUNKS:
                        tile_copy(g * per_line + c + AHEAD).start()
                    tile_copy(g * per_line + c).wait()
                    feed_many(tiles_ref, ray_ref, acc_cell, 0, lines, g, c * per_chunk, per_chunk // 8)
                    turn((g * per_line + c) * per_chunk, early)

            line(0)
            pl.when(is_reducer)(lambda: pl.semaphore_wait(barrier, n - 1))
            pl.when(is_other)(lambda: pl.semaphore_wait(barrier, chips))
            send_keys()
            for g in range(1, lines):
                line(g)

            sums = taken(acc_cell)
        send_a[step] = sums.astype(BF16).reshape(reducers, part, width)
        norm_a[step] = jnp.sum(uraw * uraw, axis=0, keepdims=True)
        send_sums(step)
        if step == 0:
            turn_rest()

        @pl.when(is_reducer)
        def _(step=step, alpha=alpha, phibar=phibar, rhobar=rhobar, coefs=coefs):
            recv_a[step, me] = send_a[step, place]
            norm_recv_a[step, me] = norm_a[step]
            if step == 0:
                prepare()
            else:
                v = vraw_ref[...] / alpha
                if step == 1:
                    w_ref[...] = v
                    update_ref[...] = jnp.zeros_like(v)
                else:
                    w = w_ref[...]
                    update_ref[...] = update_ref[...] + coefs[0] * w
                    w_ref[...] = v - coefs[1] * w
            if step == 1:
                prepare_out()

        @pl.when(is_reducer)
        def _(step=step, alpha=alpha, phibar=phibar, rhobar=rhobar):
            wait_for(norm_recv_a.at[step], n - 1, na_sem.at[step])
            wait_for(recv_a.at[step], n - 1, a_sem.at[step])
            beta = jnp.sqrt(total(jnp.sum(norm_recv_a[step], axis=0)))

            def pieces(k):
                got = recv_a[step, pl.ds(k // part, SIDE // part)].reshape(SIDE, width)
                return (jnp.concatenate([got, got], axis=1),)

            squares = []

            def use(m, value):
                span = pl.ds(m, SIDE)
                vraw = value[:, :width] / beta
                if step > 0:
                    vraw = vraw - (beta / alpha) * vraw_ref[span, :]
                vraw_ref[span, :] = vraw
                squares.append(jnp.sum(vraw * vraw * inv_ref[span, :], axis=0, keepdims=True))

            product(same_ref, pieces, use)
            norm_b[step, pl.ds(0, 1), :] = functools.reduce(jnp.add, squares)
            norm_b[step, pl.ds(1, 1), :] = jnp.broadcast_to(beta, (1, width))
            if step < steps - 1:
                own = vraw_ref[pl.ds(pl.multiple_of(quarter * group * part, 8), group * part), :]
                send_b[step] = own.astype(BF16).reshape(group, part, width)
            send_back(step, step < steps - 1)
            norm_recv_b[step, place] = norm_b[step]
            if step < steps - 1:
                recv_b[step, place] = send_b[step, lax.rem(me, group)]
            else:
                rhobar1 = jnp.sqrt(rhobar * rhobar + damping * damping)
                rho = jnp.sqrt(rhobar1 * rhobar1 + beta * beta)
                scale = (rhobar1 / rho) * ((rhobar / rhobar1) * phibar) / rho
                update = (update_ref[...] + scale * w_ref[...]) * inv_ref[...]
                update_ref[...] = update
                vraw_ref[...] = vraw_ref[...] * inv_ref[...]

                def parts(k):
                    span = pl.ds(k, SIDE)
                    x = jnp.concatenate([update_ref[span, :], vraw_ref[span, :]], axis=1)
                    high = x.astype(BF16)
                    return high, (x - high.astype(F32)).astype(BF16)

                def use_final(m, value):
                    final_ref[m // SIDE] = value

                product(out_hot, parts, use_final)
                remote(final_ref.at[0], final_recv.at[0], final_sem, me - 1).start()
            wait_for(norm_recv_b.at[step], reducers - 1, nb_sem.at[step])
            if step < steps - 1:
                wait_for(recv_b.at[step], reducers - 1, b_sem.at[step])

        @pl.when(is_other)
        def _(step=step):
            wait_for(norm_recv_b.at[step], reducers, nb_sem.at[step])
            if step < steps - 1:
                wait_for(recv_b.at[step], reducers, b_sem.at[step])

        alpha = jnp.sqrt(total(jnp.sum(norm_recv_b[step], axis=0)[:1]))
        beta = norm_recv_b[step, 0, pl.ds(1, 1), pl.ds(0, 1)]
        u = uraw / beta
        if step == 0:
            phibar = beta
            rhobar = alpha
        else:
            rhobar1 = jnp.sqrt(rhobar * rhobar + damping * damping)
            phibar = rhobar / rhobar1 * phibar
            rho = jnp.sqrt(rhobar1 * rhobar1 + beta * beta)
            cosine = rhobar1 / rho
            sine = beta / rho
            theta = sine * alpha
            rhobar = -cosine * alpha
            phi = cosine * phibar
            phibar = sine * phibar
            coefs = (phi / rho, theta / rho)

    scale = float(BLK_DEV * width * n) ** 0.5 / alpha

    def put(result):
        result_ref[pl.ds(0, BLK_DEV), :] = result[:, :width]
        result_ref[pl.ds(BLK_DEV, BLK_DEV), :] = result[:, width:] * scale

    @pl.when(is_reducer)
    def _():
        put(final_ref[1])

    @pl.when(is_other)
    def _():
        wait_for(final_recv, 1, final_sem)
        put(final_recv[0])

    @pl.when(is_reducer)
    def _():
        for k in range(QUARTERS - 1):
            wait_for(key_recv, 1, send_sem)
        for step in range(steps):
            wait_for(recv_a.at[step], chips - 1, send_sem)
            wait_for(norm_recv_a.at[step], chips - 1, send_sem)
            wait_for(norm_b.at[pl.ds(0, 1)], 1, send_sem) if group == 2 else None
            for k in range(group - 1):
                wait_for(norm_recv_b.at[step], 1, send_sem)
                if step < steps - 1:
                    wait_for(recv_b.at[step], 1, send_sem)
        wait_for(final_recv, 1, send_sem)

    @pl.when(is_other)
    def _():
        for k in range(QUARTERS):
            wait_for(key_recv, 1, send_sem)
        for step in range(steps):
            wait_for(recv_a.at[step], chips, send_sem)
            wait_for(norm_recv_a.at[step], chips, send_sem)


def per_device(n, regs, tiles, rays, tile_rows, tile_slots, tile_count, wanted):
    count, width = tiles.shape[0], tiles.shape[2]
    cap = wanted.shape[2]
    steps = ITERS + 1
    row_blocks = rays.shape[0]
    group = n // QUARTERS
    reducers = group // 2
    part = 2 * QUARTERS * cap
    slots_all = n * cap
    asked = n * part
    lines = count // width
    vmem = pl.BlockSpec(memory_space=pltpu.VMEM)
    out = jax.ShapeDtypeStruct((2 * BLK_DEV, width), F32)

    def body(*refs):
        def inner(acc_ray, acc_cell, acc_sum):
            kernel(n, regs, cap, *refs, acc_ray, acc_cell, acc_sum)

        def four(rows):
            return tuple(pltpu.ACC(q)((rows, SIDE), F32) for q in (0, 0, 1, 1))

        pl.run_scoped(
            inner, four(row_blocks), four(slots_all),
            tuple(pltpu.ACC(q)((SIDE, SIDE), F32) for q in (0, 1)),
        )

    result = pl.pallas_call(
        body,
        out_shape=out,
        in_specs=[pl.BlockSpec(memory_space=pl.ANY)] * 6,
        out_specs=vmem,
        scratch_shapes=[
            pltpu.SMEM((1,), jnp.int32),
            pltpu.VMEM(rays.shape, F32),
            pltpu.VMEM((lines, width), jnp.int32),
            pltpu.VMEM((lines, width), jnp.int32),
            pltpu.VMEM((cap, n), jnp.int32),
            pltpu.VMEM(tiles.shape, BF16),
            pltpu.VMEM(tiles.shape, BF16),
            pltpu.VMEM((2 * lines, width), jnp.int32),
            pltpu.SMEM((2 * lines, width), jnp.int32),
            pltpu.VMEM((2 * lines, width), F32),
            pltpu.SMEM((2 * lines, width), F32),
            pltpu.VMEM((max(row_blocks, slots_all) + 8, width), F32),
            pltpu.VMEM((row_blocks + 1, 16, width), BF16),
            pltpu.VMEM((slots_all + 1, 16, width), BF16),
            pltpu.VMEM((1, asked), F32),
            pltpu.VMEM((2 * QUARTERS, 1, asked), F32),
            pltpu.VMEM((8, asked), F32),
            pltpu.VMEM((asked, asked), BF16),
            pltpu.VMEM((2 * BLK_DEV, asked), BF16),
            pltpu.VMEM((asked, width), F32),
            pltpu.VMEM((asked, width), F32),
            pltpu.VMEM((asked, width), F32),
            pltpu.VMEM((asked, width), F32),
            pltpu.VMEM((2, BLK_DEV, 2 * width), F32),
            pltpu.VMEM((1, BLK_DEV, 2 * width), F32),
            pltpu.VMEM((steps, reducers, part, width), BF16),
            pltpu.VMEM((steps, n, part, width), BF16),
            pltpu.VMEM((steps, 1, width), F32),
            pltpu.VMEM((steps, n, 1, width), F32),
            pltpu.VMEM((steps - 1, group, part, width), BF16),
            pltpu.VMEM((steps - 1, reducers, part, width), BF16),
            pltpu.VMEM((steps, 2, width), F32),
            pltpu.VMEM((steps, reducers, 2, width), F32),
            pltpu.SemaphoreType.DMA((CHUNKS,)),
            pltpu.SemaphoreType.DMA((5,)),
            pltpu.SemaphoreType.DMA((2,)),
            pltpu.SemaphoreType.DMA,
            pltpu.SemaphoreType.DMA,
            pltpu.SemaphoreType.DMA((steps,)),
            pltpu.SemaphoreType.DMA((steps,)),
            pltpu.SemaphoreType.DMA((steps,)),
            pltpu.SemaphoreType.DMA((steps,)),
            pltpu.SemaphoreType.DMA,
        ],
        compiler_params=pltpu.CompilerParams(
            collective_id=0, has_side_effects=True, vmem_limit_bytes=56 * 1024 * 1024
        ),
    )(
        tile_count,
        tiles,
        rays,
        tile_rows.reshape(lines, width),
        tile_slots.reshape(lines, width),
        wanted[0].T,
    )
    return result[:BLK_DEV], result[BLK_DEV:]


def solution(mesh):
    both = ("src", "reg")
    in_specs = (
        P(both, None, None),
        P(both, None),
        P(both),
        P(both),
        P(both),
        P(both, None, None),
    )
    out_specs = (P(both, None), P(both, None))
    n = mesh.shape["src"] * mesh.shape["reg"]
    return jax.shard_map(
        functools.partial(per_device, n, mesh.shape["reg"]),
        mesh=mesh,
        in_specs=in_specs,
        out_specs=out_specs,
        check_vma=False,
    )
```

```python
import functools

import jax
import jax.numpy as jnp
from jax import lax
from jax.experimental import pallas as pl
from jax.experimental.pallas import tpu as pltpu
from jax.sharding import PartitionSpec as P

BLK_DEV = 256
ITERS = 3
damping = 0.5

QUARTERS = 4
CHUNKS = 16
AHEAD = 6
F32 = jnp.float32
BF16 = jnp.bfloat16
MESH = pl.DeviceIdType.MESH
SIDE = 256


def kernel(
    n, regs, cap,
    count_hbm, tiles_hbm, rays_hbm, rows_hbm, slots_hbm, wanted_hbm,
    result_ref,
    count_ref, rays_ref, rows_ref, slots_ref, wanted_ref,
    tiles_ref, turned_ref, index_vec, index_ref, goes_vec, goes_ref, plain_ref, ray_ref, cell_ref,
    key_send, key_recv, key_rows, same_ref, out_hot, inv_ref,
    vraw_ref, w_ref, update_ref, final_ref, final_recv,
    send_a, recv_a, norm_a, norm_recv_a, send_b, recv_b, norm_b, norm_recv_b,
    tile_sem, input_sem, index_sem, send_sem, key_sem, a_sem, na_sem, b_sem, nb_sem, final_sem,
    acc_ray, acc_cell, acc_sum,
):
    src = lax.axis_index("src")
    reg = lax.axis_index("reg")
    me = src * regs + reg
    count = tiles_ref.shape[0]
    width = tiles_ref.shape[2]
    per_chunk = count // CHUNKS
    row_blocks = rays_ref.shape[0]
    steps = ITERS + 1
    chips = n // 2
    group = n // QUARTERS
    reducers = group // 2
    part = 2 * QUARTERS * cap
    slots_all = n * cap
    asked = n * part
    chip = me // 2
    core = lax.rem(me, 2)
    quarter = me // group
    place = lax.rem(chip, reducers)
    is_reducer = core == 1
    is_other = core == 0
    iota = functools.partial(lax.broadcasted_iota, jnp.int32)

    def tile_copy(c):
        span = pl.ds(c * per_chunk, per_chunk)
        return pltpu.make_async_copy(tiles_hbm.at[span], tiles_ref.at[span], tile_sem.at[c])

    inputs = [
        pltpu.make_async_copy(a, b, input_sem.at[i])
        for i, (a, b) in enumerate((
            (count_hbm, count_ref), (rows_hbm, rows_ref), (slots_hbm, slots_ref),
            (rays_hbm, rays_ref), (wanted_hbm, wanted_ref),
        ))
    ]
    for copy in inputs:
        copy.start()
    for c in range(AHEAD):
        tile_copy(c).start()

    def at(d):
        return (d // regs, lax.rem(d, regs))

    barrier = pltpu.get_barrier_semaphore()

    def greet(d):
        pl.semaphore_signal(barrier, inc=1, device_id=at(d), device_id_type=MESH)

    @pl.loop(1, chips)
    def _(k):
        greet(lax.rem(chip + k, chips) * 2 + 1)

    @pl.when(is_reducer)
    def _():
        @pl.loop(0, chips)
        def _(k):
            greet(lax.rem(chip + k, chips) * 2)

    @pl.when(is_other)
    def _():
        greet(me + 1)

    for copy in inputs:
        copy.wait()
    lines = rows_ref.shape[0]
    tile_id = iota((lines, width), 0) * width + iota((lines, width), 1)
    live = tile_id < count_ref[0]
    slots = slots_ref[...]
    owner = slots // cap
    within = lax.rem(owner, group)
    spot = (within // 2) * part + (2 * (owner // group) + lax.rem(within, 2)) * cap + lax.rem(slots, cap)
    index_vec[:lines, :] = jnp.where(live, rows_ref[...], row_blocks)
    index_vec[lines:, :] = jnp.where(live, spot, slots_all)
    goes_vec[...] = index_vec[...].astype(F32)
    index_copies = (
        pltpu.make_async_copy(index_vec, index_ref, index_sem.at[0]),
        pltpu.make_async_copy(goes_vec, goes_ref, index_sem.at[1]),
    )
    for copy in index_copies:
        copy.start()

    asks = wanted_ref[...].astype(F32)
    lane = iota((1, asked), 1)
    asker = iota((cap, asked), 1) // part
    spread = jnp.zeros((cap, asked), F32)
    for d in range(n):
        spread = jnp.where(asker == d, asks[:, d : d + 1], spread)
    which = 2 * quarter + core
    keys = jnp.zeros((1, asked), F32)
    for k in range(cap):
        hit = lax.rem(lane, part) == which * cap + k
        keys = keys + jnp.where(hit, spread[k : k + 1] + (which * BLK_DEV).astype(F32), 0.0)
    key_send[...] = keys

    for acc in (*acc_ray, *acc_cell, *acc_sum):
        pltpu.matmul_pop(acc)

    ray_ref[row_blocks] = jnp.zeros((16, width), BF16)
    cell_ref[slots_all] = jnp.zeros((16, width), BF16)

    def spread_rows(vec_ref, value):
        plain_ref[pl.ds(0, value.shape[0]), :] = value
        for r in range(value.shape[0]):
            row = plain_ref[pl.ds(r, 8, stride=0), :]
            vec_ref[r] = jnp.concatenate([row, row], axis=0).astype(BF16)

    def left_of(vec_ref, rows_out, base_in, base_out, g, i):
        value = vec_ref[index_ref[base_in + g, i]]
        value = jnp.concatenate([value] * (rows_out // 16), axis=0)
        goes = jnp.broadcast_to(goes_ref[base_out + g, i], (16, width)).astype(BF16)
        goes = jnp.concatenate([goes] * (rows_out // 16), axis=0)
        hot = iota((rows_out, width), 0).astype(F32).astype(BF16) == goes
        return jnp.where(hot, value, jnp.zeros_like(value))

    def feed(source, vec_ref, accs, base_in, base_out, g, t, q, register):
        tile = [source[g * width + t + i] for i in range(4)]
        right = jnp.concatenate(
            [jnp.concatenate(tile[:2], axis=1), jnp.concatenate(tile[2:], axis=1)], axis=0
        )
        rows_out = accs[0].shape[0]
        left = [left_of(vec_ref, rows_out, base_in, base_out, g, t + i) for i in range(4)]
        pltpu.matmul_push_rhs(right, staging_register=register, mxu_index=q)
        pltpu.matmul_acc_lhs(
            accs[2 * q], jnp.concatenate([left[0], left[2]], axis=1), load_staged_rhs=register
        )
        pltpu.matmul_acc_lhs(accs[2 * q + 1], jnp.concatenate([left[1], left[3]], axis=1))

    def feed_many(source, vec_ref, accs, base_in, base_out, g, t, pairs):
        for i in range(pairs):
            for q in range(2):
                feed(source, vec_ref, accs, base_in, base_out, g, t + 8 * i + 4 * q, q, i % 2)

    def taken(accs):
        pieces = [pltpu.matmul_pop(acc) for acc in accs]
        return (pieces[0][:, :width] + pieces[2][:, :width]) + (
            pieces[1][:, width:] + pieces[3][:, width:]
        )

    def full_pass(source, vec_ref, accs, base_in, base_out, late=None):
        for g in range(lines):
            if late is not None and g == lines - 1:
                late()
            feed_many(source, vec_ref, accs, base_in, base_out, g, 0, width // 8)

        return taken(accs)

    def product(left_ref, right_of, use, accs=acc_sum, first=0, high=None):
        deep = left_ref.shape[1]
        high = left_ref.shape[0] if high is None else high
        tall = accs[0].shape[0]
        for m in range(0, high, 2 * tall):
            for k in range(0, deep, SIDE):
                for p, right in enumerate(right_of(k)):
                    for q in range(2):
                        span = pl.ds(pl.multiple_of(first + m + q * tall, 16), tall)
                        pltpu.matmul_push_rhs(right, staging_register=p % 2, mxu_index=q)
                        pltpu.matmul_acc_lhs(
                            accs[q], left_ref[span, pl.ds(k, SIDE)], load_staged_rhs=p % 2
                        )
            for q in range(2):
                use(m + q * tall, pltpu.matmul_pop(accs[q]))

    def remote(source, target, sem, d):
        return pltpu.make_async_remote_copy(
            src_ref=source, dst_ref=target, send_sem=send_sem, recv_sem=sem,
            device_id=at(d), device_id_type=MESH,
        )

    def wait_for(ref, number, sem):
        ref = ref.at[pl.ds(0, number)]
        pltpu.make_async_copy(ref, ref, sem).wait()

    def total(x):
        return jnp.sum(x, keepdims=True)

    def send_keys():
        for k in range(QUARTERS):
            d = lax.rem(quarter + k, QUARTERS) * group + 2 * place + 1
            copy = remote(key_send, key_recv.at[which], key_sem, d)
            if k > 0:
                copy.start()
            else:
                pl.when(is_other)(copy.start)

    def send_sums(step, norms):
        for k in range(chips - 1, -1, -1):
            to = chip ^ k if chips & (chips - 1) == 0 else lax.rem(chip + k, chips)
            d = 2 * to + 1
            if norms:
                copy = remote(norm_a.at[step], norm_recv_a.at[step, me], na_sem.at[step], d)
            else:
                source = send_a.at[step, lax.rem(to, reducers)]
                copy = remote(source, recv_a.at[step, me], a_sem.at[step], d)
            if k > 0:
                copy.start()
            else:
                pl.when(is_other)(copy.start)

    def send_back(step, norms):
        for k in range(group - 1, 0, -1):
            local = (
                lax.rem(me, group) ^ k if group & (group - 1) == 0 else lax.rem(me + k, group)
            )
            d = quarter * group + local
            if norms:
                remote(norm_b.at[step], norm_recv_b.at[step, place], nb_sem.at[step], d).start()
            else:
                remote(send_b.at[step, local], recv_b.at[step, place], b_sem.at[step], d).start()

    def prepare():
        wait_for(key_recv, 2 * QUARTERS - 1, key_sem)
        key_recv[which] = key_send[...]
        row = jnp.sum(key_recv[...], axis=0)
        key_rows[...] = jnp.broadcast_to(row, key_rows.shape)
        for b in range(0, asked, width):
            block = key_rows[:, pl.ds(b, width)]
            column = jnp.concatenate([block] * (width // 8), axis=0).T
            times = jnp.zeros((width, width), F32)
            for c in range(0, asked, width):
                equal = jnp.where(column == key_rows[pl.ds(0, 1), pl.ds(c, width)], 1.0, 0.0)
                same_ref[pl.ds(b, width), pl.ds(c, width)] = equal.astype(BF16)
                times = times + equal
            times = jnp.sum(times, axis=1, keepdims=True)
            inv_ref[pl.ds(b, width), :] = jnp.broadcast_to(1.0 / times, (width, width))

    def prepare_out():
        first = (2 * quarter * BLK_DEV).astype(F32)
        high = out_hot.shape[0]
        number = iota((high, width), 0).astype(F32) + first
        for c in range(0, asked, width):
            equal = jnp.where(number == key_rows[pl.ds(0, 1), pl.ds(c, width)], 1.0, 0.0)
            out_hot[:, pl.ds(c, width)] = equal.astype(BF16)

    early = per_chunk // 2

    def turn(first, number):
        for i in range(number):
            turned_ref[first + i] = tiles_ref[first + i].T

    def turn_rest():
        @pl.loop(0, CHUNKS)
        def _(c):
            turn(c * per_chunk + early, per_chunk - early)

    def wait_norms(step):
        @pl.when(is_reducer)
        def _():
            wait_for(norm_recv_b.at[step], reducers - 1, nb_sem.at[step])

        @pl.when(is_other)
        def _():
            wait_for(norm_recv_b.at[step], reducers, nb_sem.at[step])

    alpha = phibar = rhobar = None
    coefs = None
    uraw = rays_ref[...]
    for step in range(steps):
        if step > 0:
            spread_rows(cell_ref, recv_b[step - 1].reshape(slots_all, width).astype(F32))
            forward = full_pass(
                turned_ref, cell_ref, acc_ray, lines, 0, functools.partial(wait_norms, step - 1)
            )
            alpha = jnp.sqrt(total(jnp.sum(norm_recv_b[step - 1], axis=0)[:1]))
            beta = norm_recv_b[step - 1, 0, pl.ds(1, 1), pl.ds(0, 1)]
            if step == 1:
                phibar = beta
                rhobar = alpha
            else:
                rhobar1 = jnp.sqrt(rhobar * rhobar + damping * damping)
                phibar = rhobar / rhobar1 * phibar
                rho = jnp.sqrt(rhobar1 * rhobar1 + beta * beta)
                cosine = rhobar1 / rho
                sine = beta / rho
                theta = sine * alpha
                rhobar = -cosine * alpha
                phi = cosine * phibar
                phibar = sine * phibar
                coefs = (phi / rho, theta / rho)
            uraw = forward * (1.0 / alpha) - (alpha / beta) * uraw
            norm_a[step] = jnp.sum(uraw * uraw, axis=0, keepdims=True)
            send_sums(step, True)
            spread_rows(ray_ref, uraw)
            sums = full_pass(tiles_ref, ray_ref, acc_cell, 0, lines)
        else:
            norm_a[step] = jnp.sum(uraw * uraw, axis=0, keepdims=True)
            spread_rows(ray_ref, uraw)
            for copy in index_copies:
                copy.wait()
            per_line = width // per_chunk

            def line(g):
                for c in range(per_line):
                    if g * per_line + c + AHEAD < CHUNKS:
                        tile_copy(g * per_line + c + AHEAD).start()
                    tile_copy(g * per_line + c).wait()
                    feed_many(tiles_ref, ray_ref, acc_cell, 0, lines, g, c * per_chunk, per_chunk // 8)
                    turn((g * per_line + c) * per_chunk, early)

            line(0)
            pl.when(is_reducer)(lambda: pl.semaphore_wait(barrier, n - 1))
            pl.when(is_other)(lambda: pl.semaphore_wait(barrier, chips))
            send_keys()
            send_sums(step, True)
            for g in range(1, lines):
                line(g)
            sums = taken(acc_cell)
        send_a[step] = sums.astype(BF16).reshape(reducers, part, width)
        send_sums(step, False)
        if step == 0:
            turn_rest()

        @pl.when(is_reducer)
        def _(step=step, alpha=alpha, phibar=phibar, rhobar=rhobar, coefs=coefs):
            recv_a[step, me] = send_a[step, place]
            norm_recv_a[step, me] = norm_a[step]
            if step == 0:
                prepare()
            else:
                v = vraw_ref[...] / alpha
                if step == 1:
                    w_ref[...] = v
                    update_ref[...] = jnp.zeros_like(v)
                else:
                    w = w_ref[...]
                    update_ref[...] = update_ref[...] + coefs[0] * w
                    w_ref[...] = v - coefs[1] * w
            if step == 1:
                prepare_out()
            wait_for(norm_recv_a.at[step], n - 1, na_sem.at[step])
            beta = jnp.sqrt(total(jnp.sum(norm_recv_a[step], axis=0)))
            over = 1.0 / beta
            back = None if step == 0 else beta / alpha
            wait_for(recv_a.at[step], n - 1, a_sem.at[step])

            def pieces(k):
                got = recv_a[step, pl.ds(k // part, SIDE // part)].reshape(SIDE, width)
                return (jnp.concatenate([got, got], axis=1),)

            def vraw_of(span, value):
                vraw = value[:, :width] * over
                if step > 0:
                    vraw = vraw - back * vraw_ref[span, :]
                return vraw

            if step < steps - 1:
                tall = acc_ray[0].shape[0]
                own = quarter * group * part

                def use_own(m, value):
                    span = pl.ds(pl.multiple_of(own + m, 16), tall)
                    vraw = vraw_of(span, value).astype(BF16)
                    send_b[step, pl.ds(m // part, tall // part)] = vraw.reshape(
                        tall // part, part, width
                    )

                product(
                    same_ref, pieces, use_own, (acc_ray[0], acc_ray[2]), own, group * part
                )
                send_back(step, False)
            squares = []

            def use(m, value):
                span = pl.ds(m, SIDE)
                vraw = vraw_of(span, value)
                vraw_ref[span, :] = vraw
                squares.append(jnp.sum(vraw * vraw * inv_ref[span, :], axis=0, keepdims=True))

            product(same_ref, pieces, use)
            norm_b[step, pl.ds(0, 1), :] = functools.reduce(jnp.add, squares)
            norm_b[step, pl.ds(1, 1), :] = jnp.broadcast_to(beta, (1, width))
            send_back(step, True)
            norm_recv_b[step, place] = norm_b[step]
            if step < steps - 1:
                recv_b[step, place] = send_b[step, lax.rem(me, group)]
                wait_for(recv_b.at[step], reducers - 1, b_sem.at[step])
            else:
                rhobar1 = jnp.sqrt(rhobar * rhobar + damping * damping)
                rho = jnp.sqrt(rhobar1 * rhobar1 + beta * beta)
                scale = (rhobar1 / rho) * ((rhobar / rhobar1) * phibar) / rho
                update = (update_ref[...] + scale * w_ref[...]) * inv_ref[...]
                update_ref[...] = update
                vraw_ref[...] = vraw_ref[...] * inv_ref[...]

                def parts(k):
                    span = pl.ds(k, SIDE)
                    x = jnp.concatenate([update_ref[span, :], vraw_ref[span, :]], axis=1)
                    high = x.astype(BF16)
                    return high, (x - high.astype(F32)).astype(BF16)

                def use_final(m, value):
                    final_ref[m // SIDE] = value

                product(out_hot, parts, use_final)
                remote(final_ref.at[0], final_recv.at[0], final_sem, me - 1).start()

        if step < steps - 1:

            @pl.when(is_other)
            def _(step=step):
                wait_for(recv_b.at[step], reducers, b_sem.at[step])

    wait_norms(steps - 1)
    alpha = jnp.sqrt(total(jnp.sum(norm_recv_b[steps - 1], axis=0)[:1]))
    scale = float(BLK_DEV * width * n) ** 0.5 / alpha

    def put(result):
        result_ref[pl.ds(0, BLK_DEV), :] = result[:, :width]
        result_ref[pl.ds(BLK_DEV, BLK_DEV), :] = result[:, width:] * scale

    @pl.when(is_reducer)
    def _():
        put(final_ref[1])

    @pl.when(is_other)
    def _():
        wait_for(final_recv, 1, final_sem)
        put(final_recv[0])

    @pl.when(is_reducer)
    def _():
        for k in range(QUARTERS - 1):
            wait_for(key_recv, 1, send_sem)
        for step in range(steps):
            wait_for(recv_a.at[step], chips - 1, send_sem)
            wait_for(norm_recv_a.at[step], chips - 1, send_sem)
            for k in range(group - 1):
                wait_for(norm_recv_b.at[step], 1, send_sem)
                if step < steps - 1:
                    wait_for(recv_b.at[step], 1, send_sem)
        wait_for(final_recv, 1, send_sem)

    @pl.when(is_other)
    def _():
        for k in range(QUARTERS):
            wait_for(key_recv, 1, send_sem)
        for step in range(steps):
            wait_for(recv_a.at[step], chips, send_sem)
            wait_for(norm_recv_a.at[step], chips, send_sem)


def per_device(n, regs, tiles, rays, tile_rows, tile_slots, tile_count, wanted):
    count, width = tiles.shape[0], tiles.shape[2]
    cap = wanted.shape[2]
    steps = ITERS + 1
    row_blocks = rays.shape[0]
    group = n // QUARTERS
    reducers = group // 2
    part = 2 * QUARTERS * cap
    slots_all = n * cap
    asked = n * part
    lines = count // width
    vmem = pl.BlockSpec(memory_space=pltpu.VMEM)
    out = jax.ShapeDtypeStruct((2 * BLK_DEV, width), F32)

    def body(*refs):
        def inner(acc_ray, acc_cell, acc_sum):
            kernel(n, regs, cap, *refs, acc_ray, acc_cell, acc_sum)

        def four(rows):
            return tuple(pltpu.ACC(q)((rows, SIDE), F32) for q in (0, 0, 1, 1))

        pl.run_scoped(
            inner, four(row_blocks), four(slots_all),
            tuple(pltpu.ACC(q)((SIDE, SIDE), F32) for q in (0, 1)),
        )

    result = pl.pallas_call(
        body,
        out_shape=pltpu.VMEM((2 * BLK_DEV, width), F32),
        in_specs=[pl.BlockSpec(memory_space=pl.ANY)] * 6,
        out_specs=vmem,
        scratch_shapes=[
            pltpu.SMEM((1,), jnp.int32),
            pltpu.VMEM(rays.shape, F32),
            pltpu.VMEM((lines, width), jnp.int32),
            pltpu.VMEM((lines, width), jnp.int32),
            pltpu.VMEM((cap, n), jnp.int32),
            pltpu.VMEM(tiles.shape, BF16),
            pltpu.VMEM(tiles.shape, BF16),
            pltpu.VMEM((2 * lines, width), jnp.int32),
            pltpu.SMEM((2 * lines, width), jnp.int32),
            pltpu.VMEM((2 * lines, width), F32),
            pltpu.SMEM((2 * lines, width), F32),
            pltpu.VMEM((max(row_blocks, slots_all) + 8, width), F32),
            pltpu.VMEM((row_blocks + 1, 16, width), BF16),
            pltpu.VMEM((slots_all + 1, 16, width), BF16),
            pltpu.VMEM((1, asked), F32),
            pltpu.VMEM((2 * QUARTERS, 1, asked), F32),
            pltpu.VMEM((8, asked), F32),
            pltpu.VMEM((asked, asked), BF16),
            pltpu.VMEM((2 * BLK_DEV, asked), BF16),
            pltpu.VMEM((asked, width), F32),
            pltpu.VMEM((asked, width), F32),
            pltpu.VMEM((asked, width), F32),
            pltpu.VMEM((asked, width), F32),
            pltpu.VMEM((2, BLK_DEV, 2 * width), F32),
            pltpu.VMEM((1, BLK_DEV, 2 * width), F32),
            pltpu.VMEM((steps, reducers, part, width), BF16),
            pltpu.VMEM((steps, n, part, width), BF16),
            pltpu.VMEM((steps, 1, width), F32),
            pltpu.VMEM((steps, n, 1, width), F32),
            pltpu.VMEM((steps - 1, group, part, width), BF16),
            pltpu.VMEM((steps - 1, reducers, part, width), BF16),
            pltpu.VMEM((steps, 2, width), F32),
            pltpu.VMEM((steps, reducers, 2, width), F32),
            pltpu.SemaphoreType.DMA((CHUNKS,)),
            pltpu.SemaphoreType.DMA((5,)),
            pltpu.SemaphoreType.DMA((2,)),
            pltpu.SemaphoreType.DMA,
            pltpu.SemaphoreType.DMA,
            pltpu.SemaphoreType.DMA((steps,)),
            pltpu.SemaphoreType.DMA((steps,)),
            pltpu.SemaphoreType.DMA((steps,)),
            pltpu.SemaphoreType.DMA((steps,)),
            pltpu.SemaphoreType.DMA,
        ],
        compiler_params=pltpu.CompilerParams(
            collective_id=0, has_side_effects=True, vmem_limit_bytes=56 * 1024 * 1024
        ),
    )(
        tile_count,
        tiles,
        rays,
        tile_rows.reshape(lines, width),
        tile_slots.reshape(lines, width),
        wanted[0].T,
    )
    return result[:BLK_DEV], result[BLK_DEV:]


def solution(mesh):
    both = ("src", "reg")
    in_specs = (
        P(both, None, None),
        P(both, None),
        P(both),
        P(both),
        P(both),
        P(both, None, None),
    )
    out_specs = (P(both, None), P(both, None))
    n = mesh.shape["src"] * mesh.shape["reg"]
    return jax.shard_map(
        functools.partial(per_device, n, mesh.shape["reg"]),
        mesh=mesh,
        in_specs=in_specs,
        out_specs=out_specs,
        check_vma=False,
    )
```
